32 devices in a mesh: dp: 4 (over z), vocab: 8 (over y, x, core).
Axes of the slice: x: 2, y: 2, z: 4, core: 2. Of those that a mesh axis runs over, the one named last changes fastest.
Arguments:
- query_hidden: bfloat16 [128, 4096], P('dp', 'vocab'), may hold values from -6 to 6
- passage_hidden_rows: bfloat16 [384, 4096], P('dp', 'vocab'), may hold values from -6 to 6
- head_weight: bfloat16 [4096, 128256], P(None, ('dp', 'vocab')), may hold values from -0.09375 to 0.09375
- head_bias: bfloat16 [128256], P(('dp', 'vocab')), may hold values from -4 to 4
- query_mask: int32 [8, 16], P('dp'), may hold values from 0 to 1, as said below
- passage_mask: int32 [8, 48], P('dp'), may hold values from 0 to 1, as said below
- positives: int32 [8], P('dp'), may hold values from 0 to 7, as said below
Outputs:
- loss: float32 [], replicated
- query_grad: bfloat16 [128, 4096], P('dp', 'vocab')
- passage_grad: bfloat16 [384, 4096], P('dp', 'vocab')
The draws below stay inside these ranges and needn't reach their ends.
Inputs may be any that keep to these rules, and one draw needn't show every extreme that they name: `query_mask`: each row holds 4 or more ones from its first token on, then zeros. `passage_mask`: each row holds 12 or more ones from its first token on, then zeros. `positives`: query i's positive is a passage of its own group: it lies in [(i // 2) * 2, (i // 2 + 1) * 2).
All inputs are finite; a program needn't handle non-finite values.
Results may differ from the reference program's by a relative error of at most 0.013.
Values may be sent and summed in bfloat16 or wider, within the bound.
A program may use at most 128 MiB of HBM per device.

```python
import jax
import jax.numpy as jnp
from jax import lax

D = 4096
VOCAB = 128256
LQ = 16
LP = 48
QUERY_GROUP_SIZE = 2
PAS_GRP = 2
QUERIES = 8
PASSAGES = 8


def prefix_mask(key, text_series, span_extent):
    kept_tokens = jax.random.randint(key, (text_series, 1), max(span_extent // 4, 1), span_extent + 1)
    return (jnp.arange(span_extent, dtype=jnp.int32)[None, :] < kept_tokens).astype(jnp.int32)


def draw_query_mask(key, part):
    return prefix_mask(jax.random.fold_in(key, 11), QUERIES, LQ)


def draw_passage_mask(key, part):
    return prefix_mask(jax.random.fold_in(key, 13), PASSAGES, LP)


def draw_positives(key, part):
    offsets = jax.random.randint(jax.random.fold_in(key, 17), (QUERIES,), 0, PAS_GRP)
    return jnp.arange(QUERIES, dtype=jnp.int32) // QUERY_GROUP_SIZE * PAS_GRP + offsets


def shard_levels(own_key, extent, cuts, low, top_value):
    loudness = 1.0
    for axis_at, blocks in cuts:
        steps = jax.random.uniform(jax.random.fold_in(jax.random.fold_in(own_key, 6), axis_at), (blocks,), jnp.float32, low / len(cuts), top_value / len(cuts))
        loudness = loudness * jnp.repeat(jnp.exp(steps), extent[axis_at] // blocks).reshape((-1,) + (1,) * (len(extent) - 1 - axis_at))
    return loudness


def scatter_about(key, dims, scale, limit, split=(), held_as=jnp.bfloat16):
    entries = scale * jax.random.normal(key, dims, jnp.float32)
    if split:
        entries = entries * shard_levels(key, dims, split, -0.22, 0.18)
    return jnp.clip(entries, -limit, limit).astype(held_as)


def setup_inputs(seed: int = 0) -> dict:
    splits = jax.random.split(jax.random.key(seed), 8)
    query_hidden = scatter_about(splits[0], (QUERIES * LQ, D), 1.0, 6.0, ((0, 4), (1, 8)))
    passage_hidden_rows = scatter_about(splits[1], (PASSAGES * LP, D), 1.0, 6.0, ((0, 4), (1, 8)))
    head_weight = scatter_about(splits[2], (D, VOCAB), D ** -0.5, 0.09375, ((1, 32),))
    head_bias = scatter_about(splits[3], (VOCAB,), 1.0, 4.0, ((0, 32),))
    query_mask = draw_query_mask(jax.random.fold_in(splits[7], 71), 0)
    passage_mask = draw_passage_mask(jax.random.fold_in(splits[7], 71), 0)
    positives = draw_positives(jax.random.fold_in(splits[7], 71), 0)
    return {"query_hidden": query_hidden, "passage_hidden_rows": passage_hidden_rows, "head_weight": head_weight, "head_bias": head_bias, "query_mask": query_mask, "passage_mask": passage_mask, "positives": positives}


logit_divisor = 50.0
loss_scale = 1048576.0
epsilon = 1e-06

def pool_tokens(raw_scores_matrix, token_mask):
    text_series, span_extent = token_mask.shape
    lexical_response = jnp.log1p(jax.nn.softplus(raw_scores_matrix)).reshape(text_series, span_extent, -1)
    retained_flag = token_mask.astype(jnp.float32)
    term_importance = retained_flag[:, :, None] * jnp.exp(lexical_response)
    weight_sum = lax.optimization_barrier(jnp.sum(term_importance, axis=1))
    term_total_count = lax.optimization_barrier(jnp.sum(retained_flag, axis=1))[:, None]
    return (jnp.log(weight_sum / term_total_count), term_importance, weight_sum)

def spread(rep_grad, term_importance, weight_sum, raw_scores_matrix):
    text_series, span_extent, columns = term_importance.shape
    token_share = term_importance / weight_sum[:, None, :] * rep_grad[:, None, :]
    act_slope = jax.nn.sigmoid(raw_scores_matrix) / (1.0 + jax.nn.softplus(raw_scores_matrix))
    return token_share.reshape(text_series * span_extent, columns) * act_slope

def contrast(dots, query_sq, passage_sq, targets):
    question_length_measure = jnp.sqrt(query_sq + epsilon)
    document_length_measure = jnp.sqrt(passage_sq + epsilon)
    multiplier_coefficient = logit_divisor / (question_length_measure[:, None] * document_length_measure[None, :])
    scores = dots * multiplier_coefficient
    exp_scores = jnp.exp(scores)
    exp_total = lax.optimization_barrier(jnp.sum(exp_scores, axis=1))
    onehot = (targets[:, None] == jnp.arange(dots.shape[1], dtype=jnp.int32)[None, :]).astype(jnp.float32)
    loss = jnp.mean(jnp.log(exp_total) - lax.optimization_barrier(jnp.sum(onehot * scores, axis=1)))
    score_grad = (exp_scores / exp_total[:, None] - onehot) * (loss_scale / dots.shape[0])
    dots_grad = score_grad * multiplier_coefficient
    score_back = score_grad * scores
    query_coef = -lax.optimization_barrier(jnp.sum(score_back, axis=1)) / (query_sq + epsilon)
    passage_coef = -lax.optimization_barrier(jnp.sum(score_back, axis=0)) / (passage_sq + epsilon)
    return (loss, dots_grad, query_coef, passage_coef)

def reference(query_hidden, passage_hidden_rows, head_weight, head_bias, query_mask, passage_mask, positives):
    blocks = 8
    vocab_cols = VOCAB // blocks

    def weight_at(block_index):
        offset = (block_index * vocab_cols).astype(jnp.int32)
        weight_block = lax.dynamic_slice_in_dim(head_weight, offset, vocab_cols, 1)
        bias_block = lax.dynamic_slice_in_dim(head_bias, offset, vocab_cols, 0).astype(jnp.float32)
        return (weight_block, bias_block)

    def forward(block_index):
        weight_block, bias_block = weight_at(block_index)
        query_logits = jnp.dot(query_hidden, weight_block, preferred_element_type=jnp.float32) + bias_block
        passage_logits = jnp.dot(passage_hidden_rows, weight_block, preferred_element_type=jnp.float32) + bias_block
        query_rep = pool_tokens(query_logits, query_mask)[0]
        passage_rep = pool_tokens(passage_logits, passage_mask)[0]
        dots = jnp.einsum('qv,pv->qp', query_rep, passage_rep, precision=lax.Precision.HIGHEST)
        return (dots, lax.optimization_barrier(jnp.sum(query_rep * query_rep, axis=1)), lax.optimization_barrier(jnp.sum(passage_rep * passage_rep, axis=1)), query_logits, passage_logits)
    block_dots, block_qsq, block_psq, query_logits, passage_logits = lax.map(forward, jnp.arange(blocks, dtype=jnp.int32))
    loss, dots_grad, query_coef, passage_coef = contrast(lax.optimization_barrier(jnp.sum(block_dots, axis=0)), lax.optimization_barrier(jnp.sum(block_qsq, axis=0)), lax.optimization_barrier(jnp.sum(block_psq, axis=0)), positives)

    def backward(grad_sums, inputs):
        block_index, query_block_rows, passage_block = inputs
        weight_block, bias_block = weight_at(block_index)
        query_rep, query_weight, query_total = pool_tokens(query_block_rows, query_mask)
        passage_rep, passage_weight, passage_total = pool_tokens(passage_block, passage_mask)
        query_rep_grad = jnp.einsum('qp,pv->qv', dots_grad, passage_rep, precision=lax.Precision.HIGHEST) + query_coef[:, None] * query_rep
        passage_rep_grad = jnp.einsum('qp,qv->pv', dots_grad, query_rep, precision=lax.Precision.HIGHEST) + passage_coef[:, None] * passage_rep
        query_dlog = spread(query_rep_grad, query_weight, query_total, query_block_rows).astype(jnp.bfloat16)
        passage_dlog = spread(passage_rep_grad, passage_weight, passage_total, passage_block).astype(jnp.bfloat16)
        contract = (((1,), (1,)), ((), ()))
        query_sum = grad_sums[0] + lax.dot_general(query_dlog, weight_block, contract, preferred_element_type=jnp.float32)
        passage_sum = grad_sums[1] + lax.dot_general(passage_dlog, weight_block, contract, preferred_element_type=jnp.float32)
        return ((query_sum, passage_sum), None)
    zero_pair = (jnp.zeros(query_hidden.shape, jnp.float32), jnp.zeros(passage_hidden_rows.shape, jnp.float32))
    grad_pair, unused = lax.scan(backward, zero_pair, (jnp.arange(blocks, dtype=jnp.int32), query_logits, passage_logits))
    return (loss, grad_pair[0].astype(jnp.bfloat16), grad_pair[1].astype(jnp.bfloat16))
```

```python
import functools

import jax
import jax.numpy as jnp
from jax import lax
from jax.experimental import pallas as pl
from jax.experimental.pallas import tpu as pltpu
from jax.sharding import PartitionSpec as P

logit_divisor = 50.0
loss_scale = 1048576.0
epsilon = 1e-06
lanes = 128
MESH = pl.DeviceIdType.MESH


def aligned(at, step):
    return at if isinstance(at, int) else pl.multiple_of(at, step)


def contrast(stats, targets, n):
    dots = stats[:, :n]
    eye = lax.broadcasted_iota(jnp.int32, (n, n), 0) == lax.broadcasted_iota(jnp.int32, (n, n), 1)
    q_row = jnp.sum(jnp.where(eye, stats[:, n : n + 1], 0.0), axis=0, keepdims=True)
    p_col = stats[:, n + 1 : n + 2]
    scaling = logit_divisor / (jnp.sqrt(q_row + epsilon) * jnp.sqrt(p_col + epsilon))
    scores = dots * scaling
    exp_scores = jnp.exp(scores)
    exp_total = jnp.sum(exp_scores, axis=0, keepdims=True)
    index = lax.broadcasted_iota(jnp.int32, (n, n), 0).astype(jnp.float32)
    onehot = (targets == index).astype(jnp.float32)
    losses = jnp.log(exp_total) - jnp.sum(onehot * scores, axis=0, keepdims=True)
    loss = jnp.sum(losses, axis=1, keepdims=True) / n
    score_grad = (exp_scores / exp_total - onehot) * (loss_scale / n)
    dots_grad = score_grad * scaling
    back = score_grad * scores
    q_coef = -jnp.sum(back, axis=0, keepdims=True) / (q_row + epsilon)
    p_coef = -jnp.sum(back, axis=1, keepdims=True) / (p_col + epsilon)

    def column(row):
        return jnp.sum(jnp.where(eye, row, 0.0), axis=1, keepdims=True)

    for_q = [column(dots_grad[j : j + 1]) for j in range(n)]
    for_p = [dots_grad[:, i : i + 1] for i in range(n)]
    return loss, for_q, for_p, column(q_coef), p_coef


def head_kernel(
    groups, blocks, seq_q, len_q, seq_p, len_p, cols, tile, unroll,
    q_ref, p_ref, w_ref, bias_ref, qm_ref, pm_ref, pos_ref, loss_ref, qo_ref, po_ref,
    x, wv, sig, keep, sums, rep, inv, acc, small, smalls, counts, goal, stat_v, stat_g,
    away, pair, mine, pooled, relayed, froms, turned, last,
    w_sem, own_sem, z_send, small_send, small_recv, x_send, x_recv,
    sv_send, sv_recv, sg_send, sg_recv, pair_send, pair_recv, plane_send, relay_recv, from_recv,
    last_send, last_recv,
):
    g, v = lax.axis_index("dp"), lax.axis_index("vocab")
    chip, core = lax.div(v, 2), lax.rem(v, 2)
    partner = v + 1 - 2 * core
    half = blocks // 2
    tree = half == 4
    rows_q = seq_q * len_q
    rows, width = rows_q + seq_p * len_p, q_ref.shape[1]
    queries, tiles = groups * seq_q, x.shape[1] and sig.shape[1] // tile
    seqs = seq_q + seq_p

    def to_chip(r):
        if tree:
            return lax.rem(lax.div(chip, 2) + r // 2, 2) * 2 + lax.rem(chip + r % 2, 2)
        return lax.rem(chip + r, half)

    def from_chip(r):
        return to_chip(r) if tree else lax.rem(chip + half - r, half)

    def vocab_of(c):
        return c * 2 + core

    started = []

    def go(src, dst, send_sem, recv_sem, peer, like):
        pltpu.make_async_remote_copy(
            src_ref=src, dst_ref=dst, send_sem=send_sem[0].at[send_sem[1:]], recv_sem=recv_sem,
            device_id=peer, device_id_type=MESH,
        ).start()
        started.append((send_sem, like))

    def arrived(dst, recv_sem, peer):
        pltpu.make_async_remote_copy(
            src_ref=dst, dst_ref=dst, send_sem=z_send.at[0], recv_sem=recv_sem,
            device_id=peer, device_id_type=MESH,
        ).wait_recv()

    def drain():
        for send_sem, like in started:
            pltpu.make_async_remote_copy(
                src_ref=like[0].at[like[1:]], dst_ref=like[0].at[like[1:]],
                send_sem=send_sem[0].at[send_sem[1:]], recv_sem=z_send.at[0],
                device_id=(g, partner), device_id_type=MESH,
            ).wait_send()
        started.clear()

    loads = []
    stored = w_ref.shape[0]
    for t in range(tiles):
        n = min(tile, stored - t * tile)
        at = pl.ds(t * tile, n)
        loads.append(pltpu.make_async_copy(w_ref.at[at], wv.at[at], w_sem.at[t]))

    def block(vs, gs, part=None):
        n = rows if part is None else rows // 2
        at = gs * rows if part is None else gs * rows + part * n
        return x.at[
            pl.ds(aligned(at, n), n), pl.ds(aligned(vs * width, width), width)
        ]

    full = (x, pl.ds(0, rows), pl.ds(0, width))
    part_of = (x, pl.ds(0, rows // 2), pl.ds(0, width))
    own_cols = pl.ds(aligned(v * width, width), width)
    own_q = pltpu.make_async_copy(
        q_ref, x.at[pl.ds(aligned(g * rows, rows), rows_q), own_cols], own_sem.at[0]
    )
    own_p = pltpu.make_async_copy(
        p_ref,
        x.at[pl.ds(aligned(g * rows + rows_q, rows_q), rows - rows_q), own_cols],
        own_sem.at[1],
    )
    own_q.start()
    own_p.start()
    for load in loads:
        load.start()

    along_dp = [(lax.rem(g + k, groups), v) for k in range(1, groups)]
    along_vocab = [(g, lax.rem(v + k, blocks)) for k in range(1, blocks)]
    barrier = pltpu.get_barrier_semaphore()
    for peer in along_dp + along_vocab:
        pl.semaphore_signal(barrier, inc=1, device_id=peer, device_id_type=MESH)

    small[...] = jnp.zeros(small.shape, small.dtype)
    small[:seq_q, :len_q] = qm_ref[...]
    small[seq_q:seqs, :len_p] = pm_ref[...]
    lane = lax.broadcasted_iota(jnp.int32, (1, lanes), 1)
    row = jnp.zeros((1, lanes), jnp.int32)
    for i in range(seq_q):
        row = jnp.where(lane == i, pos_ref[i], row)
    small[seqs : seqs + 1] = row
    smalls[g] = small[...]
    pl.semaphore_wait(barrier, len(along_dp + along_vocab))

    pairs = groups // 2
    order = [g, g + 1 - 2 * lax.rem(g, 2)]
    bases = [lax.rem(lax.div(g, 2) + k, pairs) * 2 for k in range(pairs)]
    for base in bases[1:]:
        order += [base, base + 1]

    direct = [1, 2] if tree else list(range(1, half))

    def fan(n):
        gs = order[n]
        for k, r in enumerate(direct):
            vs = vocab_of(to_chip(r))
            go(block(v, gs), block(v, gs), (x_send, n, k), x_recv.at[v, gs, 0], (g, vs), full)
        sem = (x_send, n, half)
        go(block(v, gs), block(v, gs), sem, x_recv.at[v, gs, 0], (g, partner), full)

    def relay(n):
        gs = order[n]
        for k, r in enumerate(direct):
            vs = vocab_of(from_chip(r))
            arrived(block(vs, gs), x_recv.at[vs, gs, 0], (g, partner))
            if tree:
                to = (g, vocab_of(to_chip(3 - r)))
                part = block(vs, gs, k)
                go(part, part, (x_send, n, half + 1 + k), x_recv.at[vs, gs, k], to, part_of)
            go(
                block(vs, gs), block(vs, gs), (x_send, n, len(direct) + 3 + half + k),
                x_recv.at[vs, gs, 0], (g, partner), full,
            )

    def corner(n):
        if not tree:
            return
        gs, vs = order[n], vocab_of(to_chip(3))
        for k in range(2):
            part = block(vs, gs, k)
            arrived(part, x_recv.at[vs, gs, k], (g, partner))
            sem = (x_send, n, half + 3 + k)
            go(part, part, sem, x_recv.at[vs, gs, k], (g, partner), part_of)

    def settled(n):
        gs = order[n]
        for r in range(half):
            vs = from_chip(r) * 2 + 1 - core
            if tree and r == 3:
                for k in range(2):
                    arrived(block(vs, gs, k), x_recv.at[vs, gs, k], (g, partner))
            else:
                arrived(block(vs, gs), x_recv.at[vs, gs, 0], (g, partner))

    own_q.wait()
    own_p.wait()
    for n in range(1, groups):
        go(block(v, g), block(v, g), (z_send, n - 1), x_recv.at[v, g, 0], (order[n], v), full)
        if n == 1:
            fan(0)
    for n in range(1, groups):
        sem = (small_send, n - 1)
        go(smalls.at[g], smalls.at[g], sem, small_recv.at[g], (order[n], v), (smalls, 0))

    def reach(n):
        arrived(block(v, order[n]), x_recv.at[v, order[n], 0], (g, partner))
        fan(n)

    reach(1)
    relay(0)
    relay(1)
    for n in range(2, groups):
        reach(n)

    for n in range(1, groups):
        gs = order[n]
        arrived(smalls.at[gs], small_recv.at[gs], (g, partner))
    aim = jnp.zeros((1, lanes), jnp.float32)
    for a in range(groups):
        ints = smalls[a].astype(jnp.float32)
        ones = jnp.sum(ints, axis=1, keepdims=True)
        first = a * rows
        for s in range(seqs):
            size = len_q if s < seq_q else len_p
            held = lax.broadcasted_iota(jnp.int32, (size, lanes), 0).astype(jnp.float32)
            keep[first : first + size] = (held < ones[s : s + 1]).astype(jnp.float32)
            first += size
            at = a * seq_q + s if s < seq_q else queries + a * seq_p + s - seq_q
            counts[at : at + 1] = jnp.broadcast_to(ones[s : s + 1], (1, lanes))
        for i in range(seq_q):
            value = jnp.sum(
                jnp.where(lane == i, ints[seqs : seqs + 1], 0.0), axis=1, keepdims=True
            )
            aim = jnp.where(lane == a * seq_q + i, value, aim)
    goal[...] = aim

    corner(0)
    corner(1)
    settled(0)
    settled(1)

    some = 2 * rows

    def product(base, t, slot):
        acc[slot] = lax.dot_general(
            x[pl.ds(aligned(base * rows, some), some)],
            wv[pl.ds(aligned(t * tile, tile), tile)],
            (((1,), (1,)), ((), ())),
            preferred_element_type=jnp.float32,
        )

    def pool(base, t, slot):
        at = pl.ds(aligned(t * tile, tile), tile)
        bias = bias_ref[:, at]
        for m in range(2):
            first = m * rows
            for s in range(seqs):
                size = len_q if s < seq_q else len_p
                step = 16 if size % 16 == 0 else size
                total = None
                for r in range(first, first + size, step):
                    logits = acc[slot, r : r + step] + bias
                    low = jnp.exp(-jnp.abs(logits))
                    grown = 1.0 + low
                    soft = jnp.maximum(logits, 0.0) + jnp.log(grown)
                    place = pl.ds(aligned(base * rows + r, step), step)
                    kept = jnp.concatenate([keep[place]] * (tile // lanes), axis=1)
                    weight = kept * (1.0 + soft)
                    share = kept * (jnp.where(logits >= 0.0, 1.0, low) / grown)
                    sig[place, at] = share.astype(sig.dtype)
                    total = weight if total is None else total + weight
                sums[base + m, s : s + 1, at] = jnp.sum(total, axis=0, keepdims=True)
                first += size

    rounds = tiles // unroll
    for k, base in enumerate(bases):
        events = []
        if k + 1 < pairs:
            a, b = 2 * k + 2, 2 * k + 3
            events = [(relay, a), (relay, b), (corner, a), (corner, b)]

        @pl.loop(0, rounds)
        def _(i):
            if k == 0:
                for r in range(rounds):

                    @pl.when(i == r)
                    def _():
                        for load in loads[r * unroll : (r + 1) * unroll]:
                            load.wait()

            for u in range(unroll):
                t = i * unroll + u
                product(base, t, u)
                if unroll > 1:
                    pool(base, jnp.maximum(t - 1, 0), (u - 1) % unroll)
                else:
                    pool(base, t, u)
            for e, (event, n) in enumerate(events):

                @pl.when(i == min(e, rounds - 1))
                def _():
                    event(n)

        if unroll > 1:
            pool(base, tiles - 1, unroll - 1)
        if k + 1 < pairs:
            settled(2 * k + 2)
            settled(2 * k + 3)

    parts = tile // lanes
    fold = lambda y: sum(y[:, n * lanes : (n + 1) * lanes] for n in range(parts))
    cross = [None] * queries
    squares = [None, None]
    plus = lambda a, b: b if a is None else a + b
    for t in range(tiles):
        at = slice(t * tile, (t + 1) * tile)
        valid = lax.broadcasted_iota(jnp.int32, (1, tile), 1) < cols - t * tile
        reps = []
        for kind, (low, high) in enumerate(((0, seq_q), (seq_q, seqs))):
            total = jnp.concatenate([sums[a, low:high, at] for a in range(groups)], axis=0)
            total = jnp.where(valid, total, 1.0)
            part = slice(kind * queries, (kind + 1) * queries)
            count = jnp.concatenate([counts[part]] * parts, axis=1)
            value = jnp.where(valid, jnp.log(total / count), 0.0)
            rep[part, at] = value
            inv[part, at] = 1.0 / total
            reps.append(value)
            squares[kind] = plus(squares[kind], fold(value * value))
        for i in range(queries):
            cross[i] = plus(cross[i], fold(reps[0][i : i + 1] * reps[1]))
    wide = lax.broadcasted_iota(jnp.int32, (queries, lanes), 1)
    stats = jnp.zeros((queries, lanes), jnp.float32)
    for i, piece in enumerate(cross + squares):
        stats = jnp.where(wide == i, jnp.sum(piece, axis=1, keepdims=True), stats)

    stat_v[v] = stats
    for k, peer in enumerate(along_vocab):
        go(stat_v.at[v], stat_v.at[v], (sv_send, k), sv_recv.at[v], peer, (stat_v, 0))
    for k in range(1, blocks):
        vs = lax.rem(v + blocks - k, blocks)
        arrived(stat_v.at[vs], sv_recv.at[vs], (g, partner))
    stats = stat_v[0]
    for n in range(1, blocks):
        stats = stats + stat_v[n]
    stat_g[g] = stats
    for k, peer in enumerate(along_dp):
        go(stat_g.at[g], stat_g.at[g], (sg_send, k), sg_recv.at[g], peer, (stat_g, 0))
    for k in range(1, groups):
        gs = lax.rem(g + groups - k, groups)
        arrived(stat_g.at[gs], sg_recv.at[gs], (g, partner))
    stats = stat_g[0]
    for n in range(1, groups):
        stats = stats + stat_g[n]

    loss, for_q, for_p, q_coef, p_coef = contrast(stats, goal[:, :queries], queries)
    loss_ref[...] = loss

    for_q = [jnp.broadcast_to(y, (queries, lanes)) for y in for_q + [q_coef]]
    for_p = [jnp.broadcast_to(y, (queries, lanes)) for y in for_p + [p_coef]]

    @pl.loop(0, tiles)
    def _(t):
        for n in range(parts):
            at = pl.ds(aligned(t * tile + n * lanes, lanes), lanes)
            rep_q, rep_p = rep[:queries, at], rep[queries:, at]
            grad_q, grad_p = for_q[queries] * rep_q, for_p[queries] * rep_p
            for i in range(queries):
                grad_q = grad_q + for_q[i] * rep_p[i : i + 1]
                grad_p = grad_p + for_p[i] * rep_q[i : i + 1]
            inv[:queries, at] = grad_q * inv[:queries, at]
            inv[queries:, at] = grad_p * inv[queries:, at]
        at = pl.ds(aligned(t * tile, tile), tile)
        first = 0
        for a in range(groups):
            for s in range(seqs):
                size = len_q if s < seq_q else len_p
                row = a * seq_q + s if s < seq_q else queries + a * seq_p + s - seq_q
                sig[first : first + size, at] = (
                    sig[first : first + size, at].astype(jnp.float32) * inv[row : row + 1, at]
                ).astype(sig.dtype)
                first += size

    side = groups // 2
    upper = lax.div(g, side)
    far_base, near_base = lax.rem(upper + 1, 2) * side, upper * side
    if tree:
        stages = [(3, 0), (3, 1), (1, 0), (2, 0), (1, 1), (2, 1), (0, 0), (0, 1)]
    else:
        stages = [(r, h) for r in list(range(1, half)) + [0] for h in range(2)]
    tall = side * rows

    def place(k):
        if k < side:
            return k + (1 - upper) * (side - 1 - 2 * k)
        return lax.rem(g + 1 + k - side, side)

    def group_of(k):
        return (far_base if k < side else near_base) + place(k)

    def chunk(k):
        return pl.ds(aligned(place(k) * rows, rows), rows)

    def hand_over(s):
        go(away.at[s], pair.at[s], (pair_send, s), pair_recv.at[s], (g, partner), (away, s))

    def outcome(s):
        r, h = stages[s]
        arrived(pair.at[s], pair_recv.at[s], (g, partner))
        for k in range(h * side, (h + 1) * side):
            at = chunk(k)
            value = mine[s % 2, at] + pair[s, at].astype(jnp.float32)
            if tree and (r, k % 2) in ((1, 0), (2, 1)):
                arrived(relayed.at[k], relay_recv.at[k], (g, partner))
                value = value + relayed[k].astype(jnp.float32)
            if r:
                pooled[s, at] = value.astype(pooled.dtype)
                sem = (plane_send, s, k % side)
                if tree and r == 3:
                    to = (g, vocab_of(to_chip(2 - k % 2)))
                    go(pooled.at[s, at], relayed.at[k], sem, relay_recv.at[k], to, (relayed, k))
                else:
                    to = (g, vocab_of(to_chip(r)))
                    go(pooled.at[s, at], froms.at[r, k], sem, from_recv.at[r, k], to, (relayed, k))
                continue
            for d in direct:
                arrived(froms.at[d, k], from_recv.at[d, k], (g, partner))
                value = value + froms[d, k].astype(jnp.float32)
            if k < groups - 1:
                turned[k] = value.astype(turned.dtype)
                to = (group_of(k), v)
                go(turned.at[k], last.at[g], (last_send, k), last_recv.at[g], to, (turned, k))
                continue
            for n in range(1, groups):
                gs = lax.rem(g + n, groups)
                arrived(last.at[gs], last_recv.at[gs], (gs, v))
                value = value + last[gs].astype(jnp.float32)
            qo_ref[...] = value[:rows_q].astype(qo_ref.dtype)
            po_ref[...] = value[rows_q:].astype(po_ref.dtype)

    def pick(s, values):
        found = values[0]
        for n in range(1, len(values)):
            found = lax.select(s == n, values[n], found)
        return found

    def gradient(s, ours):
        to = pick(s, [to_chip(r) for r, h in stages]) * 2 + (core if ours else 1 - core)
        base = pick(s, [near_base if h else far_base for r, h in stages])
        return lax.dot_general(
            sig[pl.ds(aligned(base * rows, tall), tall), :stored],
            wv[:stored, pl.ds(aligned(to * width, width), width)],
            (((1,), (0,)), ((), ())),
            preferred_element_type=jnp.float32,
        )

    @pl.loop(0, len(stages))
    def _(s):
        away[s] = gradient(s, False).astype(away.dtype)
        for n in range(len(stages)):

            @pl.when(s == n)
            def _():
                hand_over(n)
                if n:
                    outcome(n - 1)

        mine[lax.rem(s, 2)] = gradient(s, True)

    outcome(len(stages) - 1)
    drain()


def shards(
    query_hidden, passage_hidden_rows, head_weight, head_bias, query_mask, passage_mask, positives
):
    groups, blocks = lax.axis_size("dp"), lax.axis_size("vocab")
    seq_q, len_q = query_mask.shape
    seq_p, len_p = passage_mask.shape
    rows_q = seq_q * len_q
    rows, width = rows_q + seq_p * len_p, query_hidden.shape[1]
    depth, cols = head_weight.shape
    weight = head_weight.T
    if cols % 8:
        weight = jnp.pad(weight, ((0, -cols % 8), (0, 0)))
    tile = min(512, -(-cols // lanes) * lanes)
    tiles = -(-cols // tile)
    padded = tiles * tile
    unroll = 2 if tiles % 2 == 0 else 1
    bias = jnp.pad(head_bias.astype(jnp.float32), (0, padded - cols)).reshape(1, -1)
    queries = groups * seq_q
    seqs = queries + groups * seq_p
    half, side = blocks // 2, groups // 2
    stages = 2 * half
    held = -(-(seq_q + seq_p + 1) // 8) * 8
    everything = groups * rows
    dma, vmem = pltpu.SemaphoreType.DMA, pltpu.VMEM
    inside = pl.BlockSpec(memory_space=pltpu.VMEM)
    anywhere = pl.BlockSpec(memory_space=pl.ANY)
    bf16, f32 = jnp.bfloat16, jnp.float32
    loss, query_grad, passage_grad = pl.pallas_call(
        functools.partial(
            head_kernel, groups, blocks, seq_q, len_q, seq_p, len_p, cols, tile, unroll
        ),
        out_shape=(
            jax.ShapeDtypeStruct((1, 1), f32),
            jax.ShapeDtypeStruct((rows_q, width), bf16),
            jax.ShapeDtypeStruct((rows - rows_q, width), bf16),
        ),
        in_specs=[
            anywhere, anywhere, anywhere, inside, inside, inside,
            pl.BlockSpec(memory_space=pltpu.SMEM),
        ],
        out_specs=(inside, inside, inside),
        scratch_shapes=[
            vmem((everything, depth), bf16),
            vmem((padded, depth), bf16),
            vmem((everything, padded), bf16),
            vmem((everything, lanes), f32),
            vmem((groups, seq_q + seq_p, padded), f32),
            vmem((seqs, padded), f32),
            vmem((seqs, padded), f32),
            vmem((unroll, 2 * rows, tile), f32),
            vmem((held, lanes), jnp.int32),
            vmem((groups, held, lanes), jnp.int32),
            vmem((seqs, lanes), f32),
            vmem((1, lanes), f32),
            vmem((blocks, queries, lanes), f32),
            vmem((groups, queries, lanes), f32),
            vmem((stages, side * rows, width), bf16),
            vmem((stages, side * rows, width), bf16),
            vmem((2, side * rows, width), f32),
            vmem((stages, side * rows, width), bf16),
            vmem((groups, rows, width), bf16),
            vmem((half, groups, rows, width), bf16),
            vmem((groups, rows, width), bf16),
            vmem((groups, rows, width), bf16),
            dma((tiles,)),
            dma((2,)),
            dma((groups,)),
            dma((groups,)),
            dma((groups,)),
            dma((groups, 3 * half + 2)),
            dma((blocks, groups, 2)),
            dma((blocks,)),
            dma((blocks,)),
            dma((groups,)),
            dma((groups,)),
            dma((stages,)),
            dma((stages,)),
            dma((stages, side)),
            dma((groups,)),
            dma((half, groups)),
            dma((groups,)),
            dma((groups,)),
        ],
        compiler_params=pltpu.CompilerParams(
            collective_id=0, has_side_effects=True, vmem_limit_bytes=63 << 20
        ),
    )(
        query_hidden, passage_hidden_rows, weight, bias, query_mask, passage_mask, positives
    )
    return (loss[0, 0], query_grad, passage_grad)


def solution(mesh):
    placed = (
        P("dp", "vocab"),
        P("dp", "vocab"),
        P(None, ("dp", "vocab")),
        P(("dp", "vocab")),
        P("dp", None),
        P("dp", None),
        P("dp"),
    )
    return jax.shard_map(
        shards,
        mesh=mesh,
        in_specs=placed,
        out_specs=(P(), P("dp", "vocab"), P("dp", "vocab")),
        check_vma=False,
    )
```

```python
import functools

import jax
import jax.numpy as jnp
from jax import lax
from jax.experimental import pallas as pl
from jax.experimental.pallas import tpu as pltpu
from jax.sharding import PartitionSpec as P

logit_divisor = 50.0
loss_scale = 1048576.0
epsilon = 1e-06
lanes = 128
MESH = pl.DeviceIdType.MESH


def aligned(at, step):
    return at if isinstance(at, int) else pl.multiple_of(at, step)


def contrast(stats, targets, n):
    dots = stats[:, :n]
    eye = lax.broadcasted_iota(jnp.int32, (n, n), 0) == lax.broadcasted_iota(jnp.int32, (n, n), 1)
    q_row = jnp.sum(jnp.where(eye, stats[:, n : n + 1], 0.0), axis=0, keepdims=True)
    p_col = stats[:, n + 1 : n + 2]
    scaling = logit_divisor / (jnp.sqrt(q_row + epsilon) * jnp.sqrt(p_col + epsilon))
    scores = dots * scaling
    exp_scores = jnp.exp(scores)
    exp_total = jnp.sum(exp_scores, axis=0, keepdims=True)
    index = lax.broadcasted_iota(jnp.int32, (n, n), 0).astype(jnp.float32)
    onehot = (targets == index).astype(jnp.float32)
    losses = jnp.log(exp_total) - jnp.sum(onehot * scores, axis=0, keepdims=True)
    loss = jnp.sum(losses, axis=1, keepdims=True) / n
    score_grad = (exp_scores / exp_total - onehot) * (loss_scale / n)
    dots_grad = score_grad * scaling
    back = score_grad * scores
    q_coef = -jnp.sum(back, axis=0, keepdims=True) / (q_row + epsilon)
    p_coef = -jnp.sum(back, axis=1, keepdims=True) / (p_col + epsilon)

    def column(row):
        return jnp.sum(jnp.where(eye, row, 0.0), axis=1, keepdims=True)

    for_q = [column(dots_grad[j : j + 1]) for j in range(n)]
    for_p = [dots_grad[:, i : i + 1] for i in range(n)]
    return loss, for_q, for_p, column(q_coef), p_coef


def head_kernel(
    groups, blocks, seq_q, len_q, seq_p, len_p, cols, tile, unroll,
    q_ref, p_ref, w_ref, bias_ref, qm_ref, pm_ref, pos_ref, loss_ref, qo_ref, po_ref,
    x, wv, sig, keep, sums, rep, inv, acc, small, smalls, counts, goal, stat_v, stat_g,
    away, pair, mine, pooled, relayed, froms, turned, last,
    w_sem, own_sem, z_send, small_send, small_recv, x_send, x_recv,
    sv_send, sv_recv, sg_send, sg_recv, pair_send, pair_recv, plane_send, relay_recv, from_recv,
    last_send, last_recv,
):
    g, v = lax.axis_index("dp"), lax.axis_index("vocab")
    chip, core = lax.div(v, 2), lax.rem(v, 2)
    partner = v + 1 - 2 * core
    half = blocks // 2
    tree = half == 4
    rows_q = seq_q * len_q
    rows, width = rows_q + seq_p * len_p, q_ref.shape[1]
    queries, tiles = groups * seq_q, sig.shape[1] // tile
    seqs = seq_q + seq_p

    def to_chip(r):
        if tree:
            return lax.rem(lax.div(chip, 2) + r // 2, 2) * 2 + lax.rem(chip + r % 2, 2)
        return lax.rem(chip + r, half)

    def from_chip(r):
        return to_chip(r) if tree else lax.rem(chip + half - r, half)

    def vocab_of(c):
        return c * 2 + core

    started = []

    def go(src, dst, send_sem, recv_sem, peer, like):
        pltpu.make_async_remote_copy(
            src_ref=src, dst_ref=dst, send_sem=send_sem[0].at[send_sem[1:]], recv_sem=recv_sem,
            device_id=peer, device_id_type=MESH,
        ).start()
        started.append((send_sem, like))

    def arrived(dst, recv_sem, peer):
        pltpu.make_async_remote_copy(
            src_ref=dst, dst_ref=dst, send_sem=z_send.at[0], recv_sem=recv_sem,
            device_id=peer, device_id_type=MESH,
        ).wait_recv()

    def drain():
        for send_sem, like in started:
            pltpu.make_async_remote_copy(
                src_ref=like[0].at[like[1:]], dst_ref=like[0].at[like[1:]],
                send_sem=send_sem[0].at[send_sem[1:]], recv_sem=z_send.at[0],
                device_id=(g, partner), device_id_type=MESH,
            ).wait_send()
        started.clear()

    loads = []
    stored = w_ref.shape[0]
    for t in range(tiles):
        n = min(tile, stored - t * tile)
        at = pl.ds(t * tile, n)
        loads.append(pltpu.make_async_copy(w_ref.at[at], wv.at[at], w_sem.at[t]))

    def block(vs, gs, part=None, count=1):
        n = rows * count if part is None else rows * count // 2
        at = gs * rows if part is None else gs * rows + part * n
        return x.at[vs, pl.ds(aligned(at, rows // 2), n)]

    full = lambda count: (x, 0, pl.ds(0, rows * count))
    part_of = lambda count: (x, 0, pl.ds(0, rows * count // 2))
    own_q = pltpu.make_async_copy(
        q_ref, x.at[v, pl.ds(aligned(g * rows, rows), rows_q)], own_sem.at[0]
    )
    own_p = pltpu.make_async_copy(
        p_ref,
        x.at[v, pl.ds(aligned(g * rows + rows_q, rows_q), rows - rows_q)],
        own_sem.at[1],
    )
    own_q.start()
    own_p.start()

    along_dp = [(lax.rem(g + k, groups), v) for k in range(1, groups)]
    along_vocab = [(g, lax.rem(v + k, blocks)) for k in range(1, blocks)]
    barrier = pltpu.get_barrier_semaphore()
    for peer in along_dp + along_vocab:
        pl.semaphore_signal(barrier, inc=1, device_id=peer, device_id_type=MESH)

    small[...] = jnp.zeros(small.shape, small.dtype)
    small[:seq_q, :len_q] = qm_ref[...]
    small[seq_q:seqs, :len_p] = pm_ref[...]
    lane = lax.broadcasted_iota(jnp.int32, (1, lanes), 1)
    row = jnp.zeros((1, lanes), jnp.int32)
    for i in range(seq_q):
        row = jnp.where(lane == i, pos_ref[i], row)
    small[seqs : seqs + 1] = row
    smalls[g] = small[...]
    pl.semaphore_wait(barrier, len(along_dp + along_vocab))

    pairs = groups // 2
    order = [g, g + 1 - 2 * lax.rem(g, 2)]
    bases = [lax.rem(lax.div(g, 2) + k, pairs) * 2 for k in range(pairs)]
    for base in bases[1:]:
        order += [base, base + 1]

    direct = [1, 2] if tree else list(range(1, half))
    units = [(order[0], 1), (order[1], 1)] + [(base, 2) for base in bases[1:]]

    def fan(n):
        gs, c = units[n]
        mine_at = block(v, gs, None, c)
        for k, r in enumerate(direct):
            to = (g, vocab_of(to_chip(r)))
            go(mine_at, mine_at, (x_send, n, k), x_recv.at[v, gs, 0], to, full(c))
        to = (g, partner)
        go(mine_at, mine_at, (x_send, n, half), x_recv.at[v, gs, 1], to, full(c))

    def relay(n):
        gs, c = units[n]
        for k, r in enumerate(direct):
            vs = vocab_of(from_chip(r))
            whole = block(vs, gs, None, c)
            arrived(whole, x_recv.at[vs, gs, 0], (g, partner))
            if tree:
                to = (g, vocab_of(to_chip(3 - r)))
                part = block(vs, gs, k, c)
                sem = (x_send, n, half + 1 + k)
                go(part, part, sem, x_recv.at[vs, gs, k], to, part_of(c))
            sem = (x_send, n, len(direct) + 3 + half + k)
            go(whole, whole, sem, x_recv.at[vs, gs, 0], (g, partner), full(c))

    def corner(n):
        if not tree:
            return
        (gs, c), vs = units[n], vocab_of(to_chip(3))
        for k in range(2):
            part = block(vs, gs, k, c)
            arrived(part, x_recv.at[vs, gs, k], (g, partner))
            sem = (x_send, n, half + 3 + k)
            go(part, part, sem, x_recv.at[vs, gs, k], (g, partner), part_of(c))

    def settled(n):
        gs, c = units[n]
        for r in range(half):
            vs = from_chip(r) * 2 + 1 - core
            if tree and r == 3:
                for k in range(2):
                    arrived(block(vs, gs, k, c), x_recv.at[vs, gs, k], (g, partner))
            else:
                sem = x_recv.at[vs, gs, 0 if r else 1]
                arrived(block(vs, gs, None, c), sem, (g, partner))

    own_q.wait()
    own_p.wait()
    for n in range(1, groups):
        go(block(v, g), block(v, g), (z_send, n - 1), x_recv.at[v, g, 0], (order[n], v), full(1))
        if n == 1:
            fan(0)
    for n in range(1, groups):
        sem = (small_send, n - 1)
        go(smalls.at[g], smalls.at[g], sem, small_recv.at[g], (order[n], v), (smalls, 0))

    def reach(n):
        gs, c = units[n]
        for m in range(c):
            arrived(block(v, gs + m), x_recv.at[v, gs + m, 0], (g, partner))
        fan(n)

    def fetch(n):
        for load in loads[n * tiles // 4 : (n + 1) * tiles // 4]:
            load.start()

    fetch(0)
    reach(1)
    fetch(1)
    relay(0)
    fetch(2)
    relay(1)
    for n in range(2, len(units)):
        reach(n)
    fetch(3)

    for n in range(1, groups):
        gs = order[n]
        arrived(smalls.at[gs], small_recv.at[gs], (g, partner))
    aim = jnp.zeros((1, lanes), jnp.float32)
    for a in range(groups):
        ints = smalls[a].astype(jnp.float32)
        ones = jnp.sum(ints, axis=1, keepdims=True)
        first = a * rows
        for s in range(seqs):
            size = len_q if s < seq_q else len_p
            held = lax.broadcasted_iota(jnp.int32, (size, lanes), 0).astype(jnp.float32)
            keep[first : first + size] = (held < ones[s : s + 1]).astype(jnp.float32)
            first += size
            at = a * seq_q + s if s < seq_q else queries + a * seq_p + s - seq_q
            counts[at : at + 1] = jnp.broadcast_to(ones[s : s + 1], (1, lanes))
        for i in range(seq_q):
            value = jnp.sum(
                jnp.where(lane == i, ints[seqs : seqs + 1], 0.0), axis=1, keepdims=True
            )
            aim = jnp.where(lane == a * seq_q + i, value, aim)
    goal[...] = aim

    corner(0)
    corner(1)
    settled(0)
    settled(1)

    some = 2 * rows

    def product(base, t, slot):
        at = pl.ds(aligned(base * rows, some), some)
        acc[slot] = lax.dot_general(
            jnp.concatenate([x[n, at] for n in range(blocks)], axis=1),
            wv[pl.ds(aligned(t * tile, tile), tile)],
            (((1,), (1,)), ((), ())),
            preferred_element_type=jnp.float32,
        )

    def pool(base, t, slot):
        at = pl.ds(aligned(t * tile, tile), tile)
        bias = bias_ref[:, at]
        for m in range(2):
            first = m * rows
            for s in range(seqs):
                size = len_q if s < seq_q else len_p
                step = 16 if size % 16 == 0 else size
                total = None
                for r in range(first, first + size, step):
                    logits = acc[slot, r : r + step] + bias
                    low = jnp.exp(-jnp.abs(logits))
                    grown = 1.0 + low
                    soft = jnp.maximum(logits, 0.0) + jnp.log(grown)
                    place = pl.ds(aligned(base * rows + r, step), step)
                    kept = jnp.concatenate([keep[place]] * (tile // lanes), axis=1)
                    weight = kept * (1.0 + soft)
                    share = kept * (jnp.where(logits >= 0.0, 1.0, low) / grown)
                    sig[place, at] = share.astype(sig.dtype)
                    total = weight if total is None else total + weight
                sums[base + m, s : s + 1, at] = jnp.sum(total, axis=0, keepdims=True)
                first += size

    rounds = tiles // unroll
    for k, base in enumerate(bases):
        events = []
        if k + 1 < pairs:
            events = [(1, relay), (2, corner)]

        @pl.loop(0, rounds)
        def _(i):
            if k == 0:
                for r in range(rounds):

                    @pl.when(i == r)
                    def _():
                        for load in loads[r * unroll : (r + 1) * unroll]:
                            load.wait()

            for u in range(unroll):
                t = i * unroll + u
                product(base, t, u)
                if unroll > 1:
                    pool(base, jnp.maximum(t - 1, 0), (u - 1) % unroll)
                else:
                    pool(base, t, u)
            for at, event in events:

                @pl.when(i == min(at, rounds - 1))
                def _():
                    event(k + 2)

        if unroll > 1:
            pool(base, tiles - 1, unroll - 1)
        if k + 1 < pairs:
            settled(k + 2)

    parts = tile // lanes
    fold = lambda y: sum(y[:, n * lanes : (n + 1) * lanes] for n in range(parts))
    cross = [None] * queries
    squares = [None, None]
    plus = lambda a, b: b if a is None else a + b
    for t in range(tiles):
        at = slice(t * tile, (t + 1) * tile)
        valid = lax.broadcasted_iota(jnp.int32, (1, tile), 1) < cols - t * tile
        reps = []
        for kind, (low, high) in enumerate(((0, seq_q), (seq_q, seqs))):
            total = jnp.concatenate([sums[a, low:high, at] for a in range(groups)], axis=0)
            total = jnp.where(valid, total, 1.0)
            part = slice(kind * queries, (kind + 1) * queries)
            count = jnp.concatenate([counts[part]] * parts, axis=1)
            value = jnp.where(valid, jnp.log(total / count), 0.0)
            rep[part, at] = value
            inv[part, at] = 1.0 / total
            reps.append(value)
            squares[kind] = plus(squares[kind], fold(value * value))
        for i in range(queries):
            cross[i] = plus(cross[i], fold(reps[0][i : i + 1] * reps[1]))
    wide = lax.broadcasted_iota(jnp.int32, (queries, lanes), 1)
    stats = jnp.zeros((queries, lanes), jnp.float32)
    for i, piece in enumerate(cross + squares):
        stats = jnp.where(wide == i, jnp.sum(piece, axis=1, keepdims=True), stats)

    stat_v[v] = stats
    for k, peer in enumerate(along_vocab):
        go(stat_v.at[v], stat_v.at[v], (sv_send, k), sv_recv.at[v], peer, (stat_v, 0))
    for k in range(1, blocks):
        vs = lax.rem(v + blocks - k, blocks)
        arrived(stat_v.at[vs], sv_recv.at[vs], (g, partner))
    stats = stat_v[0]
    for n in range(1, blocks):
        stats = stats + stat_v[n]
    stat_g[g] = stats
    for k, peer in enumerate(along_dp):
        go(stat_g.at[g], stat_g.at[g], (sg_send, k), sg_recv.at[g], peer, (stat_g, 0))
    for k in range(1, groups):
        gs = lax.rem(g + groups - k, groups)
        arrived(stat_g.at[gs], sg_recv.at[gs], (g, partner))
    stats = stat_g[0]
    for n in range(1, groups):
        stats = stats + stat_g[n]

    loss, for_q, for_p, q_coef, p_coef = contrast(stats, goal[:, :queries], queries)
    loss_ref[...] = loss

    for_q = [jnp.broadcast_to(y, (queries, lanes)) for y in for_q + [q_coef]]
    for_p = [jnp.broadcast_to(y, (queries, lanes)) for y in for_p + [p_coef]]

    @pl.loop(0, tiles)
    def _(t):
        for n in range(parts):
            at = pl.ds(aligned(t * tile + n * lanes, lanes), lanes)
            rep_q, rep_p = rep[:queries, at], rep[queries:, at]
            grad_q, grad_p = for_q[queries] * rep_q, for_p[queries] * rep_p
            for i in range(queries):
                grad_q = grad_q + for_q[i] * rep_p[i : i + 1]
                grad_p = grad_p + for_p[i] * rep_q[i : i + 1]
            inv[:queries, at] = grad_q * inv[:queries, at]
            inv[queries:, at] = grad_p * inv[queries:, at]
        at = pl.ds(aligned(t * tile, tile), tile)
        first = 0
        for a in range(groups):
            for s in range(seqs):
                size = len_q if s < seq_q else len_p
                row = a * seq_q + s if s < seq_q else queries + a * seq_p + s - seq_q
                sig[first : first + size, at] = (
                    sig[first : first + size, at].astype(jnp.float32) * inv[row : row + 1, at]
                ).astype(sig.dtype)
                first += size

    side = groups // 2
    upper = lax.div(g, side)
    far_base, near_base = lax.rem(upper + 1, 2) * side, upper * side
    if tree:
        stages = [(3, 0), (3, 1), (1, 0), (2, 0), (1, 1), (2, 1), (0, 0), (0, 1)]
    else:
        stages = [(r, h) for r in list(range(1, half)) + [0] for h in range(2)]
    tall = side * rows

    def place(k):
        if k < side:
            return k + (1 - upper) * (side - 1 - 2 * k)
        return lax.rem(g + 1 + k - side, side)

    def group_of(k):
        return (far_base if k < side else near_base) + place(k)

    def chunk(k):
        return pl.ds(aligned(place(k) * rows, rows), rows)

    def hand_over(s):
        go(away.at[s], pair.at[s], (pair_send, s), pair_recv.at[s], (g, partner), (away, s))

    def outcome(s):
        r, h = stages[s]
        arrived(pair.at[s], pair_recv.at[s], (g, partner))
        for k in range(h * side, (h + 1) * side):
            at = chunk(k)
            value = mine[s % 2, at] + pair[s, at].astype(jnp.float32)
            if tree and (r, k % 2) in ((1, 0), (2, 1)):
                arrived(relayed.at[k], relay_recv.at[k], (g, partner))
                value = value + relayed[k].astype(jnp.float32)
            if r:
                pooled[s, at] = value.astype(pooled.dtype)
                sem = (plane_send, s, k % side)
                if tree and r == 3:
                    to = (g, vocab_of(to_chip(2 - k % 2)))
                    go(pooled.at[s, at], relayed.at[k], sem, relay_recv.at[k], to, (relayed, k))
                else:
                    to = (g, vocab_of(to_chip(r)))
                    go(pooled.at[s, at], froms.at[r, k], sem, from_recv.at[r, k], to, (relayed, k))
                continue
            for d in direct:
                arrived(froms.at[d, k], from_recv.at[d, k], (g, partner))
                value = value + froms[d, k].astype(jnp.float32)
            if k < groups - 1:
                turned[k] = value.astype(turned.dtype)
                to = (group_of(k), v)
                go(turned.at[k], last.at[g], (last_send, k), last_recv.at[g], to, (turned, k))
                continue
            for n in range(1, groups):
                gs = lax.rem(g + n, groups)
                arrived(last.at[gs], last_recv.at[gs], (gs, v))
                value = value + last[gs].astype(jnp.float32)
            qo_ref[...] = value[:rows_q].astype(qo_ref.dtype)
            po_ref[...] = value[rows_q:].astype(po_ref.dtype)

    def pick(s, values):
        found = values[0]
        for n in range(1, len(values)):
            found = lax.select(s == n, values[n], found)
        return found

    def gradient(s, ours):
        to = pick(s, [to_chip(r) for r, h in stages]) * 2 + (core if ours else 1 - core)
        base = pick(s, [near_base if h else far_base for r, h in stages])
        return lax.dot_general(
            sig[pl.ds(aligned(base * rows, tall), tall), :stored],
            wv[:stored, pl.ds(aligned(to * width, width), width)],
            (((1,), (0,)), ((), ())),
            preferred_element_type=jnp.float32,
        )

    @pl.loop(0, len(stages))
    def _(s):
        away[s] = gradient(s, False).astype(away.dtype)
        for n in range(len(stages)):

            @pl.when(s == n)
            def _():
                hand_over(n)
                if n:
                    outcome(n - 1)

        mine[lax.rem(s, 2)] = gradient(s, True)

    outcome(len(stages) - 1)
    drain()


def shards(
    query_hidden, passage_hidden_rows, head_weight, head_bias, query_mask, passage_mask, positives
):
    groups, blocks = lax.axis_size("dp"), lax.axis_size("vocab")
    seq_q, len_q = query_mask.shape
    seq_p, len_p = passage_mask.shape
    rows_q = seq_q * len_q
    rows, width = rows_q + seq_p * len_p, query_hidden.shape[1]
    depth, cols = head_weight.shape
    weight = head_weight.T
    if cols % 8:
        weight = jnp.pad(weight, ((0, -cols % 8), (0, 0)))
    tile = min(512, -(-cols // lanes) * lanes)
    tiles = -(-cols // tile)
    padded = tiles * tile
    unroll = 2 if tiles % 2 == 0 else 1
    bias = jnp.pad(head_bias.astype(jnp.float32), (0, padded - cols)).reshape(1, -1)
    queries = groups * seq_q
    seqs = queries + groups * seq_p
    half, side = blocks // 2, groups // 2
    stages = 2 * half
    held = -(-(seq_q + seq_p + 1) // 8) * 8
    everything = groups * rows
    dma, vmem = pltpu.SemaphoreType.DMA, pltpu.VMEM
    inside = pl.BlockSpec(memory_space=pltpu.VMEM)
    anywhere = pl.BlockSpec(memory_space=pl.ANY)
    bf16, f32 = jnp.bfloat16, jnp.float32
    loss, query_grad, passage_grad = pl.pallas_call(
        functools.partial(
            head_kernel, groups, blocks, seq_q, len_q, seq_p, len_p, cols, tile, unroll
        ),
        out_shape=(
            jax.ShapeDtypeStruct((1, 1), f32),
            jax.ShapeDtypeStruct((rows_q, width), bf16),
            jax.ShapeDtypeStruct((rows - rows_q, width), bf16),
        ),
        in_specs=[
            anywhere, anywhere, anywhere, inside, inside, inside,
            pl.BlockSpec(memory_space=pltpu.SMEM),
        ],
        out_specs=(inside, inside, inside),
        scratch_shapes=[
            vmem((blocks, everything, width), bf16),
            vmem((padded, depth), bf16),
            vmem((everything, padded), bf16),
            vmem((everything, lanes), f32),
            vmem((groups, seq_q + seq_p, padded), f32),
            vmem((seqs, padded), f32),
            vmem((seqs, padded), f32),
            vmem((unroll, 2 * rows, tile), f32),
            vmem((held, lanes), jnp.int32),
            vmem((groups, held, lanes), jnp.int32),
            vmem((seqs, lanes), f32),
            vmem((1, lanes), f32),
            vmem((blocks, queries, lanes), f32),
            vmem((groups, queries, lanes), f32),
            vmem((stages, side * rows, width), bf16),
            vmem((stages, side * rows, width), bf16),
            vmem((2, side * rows, width), f32),
            vmem((stages, side * rows, width), bf16),
            vmem((groups, rows, width), bf16),
            vmem((half, groups, rows, width), bf16),
            vmem((groups, rows, width), bf16),
            vmem((groups, rows, width), bf16),
            dma((tiles,)),
            dma((2,)),
            dma((groups,)),
            dma((groups,)),
            dma((groups,)),
            dma((groups, 3 * half + 2)),
            dma((blocks, groups, 2)),
            dma((blocks,)),
            dma((blocks,)),
            dma((groups,)),
            dma((groups,)),
            dma((stages,)),
            dma((stages,)),
            dma((stages, side)),
            dma((groups,)),
            dma((half, groups)),
            dma((groups,)),
            dma((groups,)),
        ],
        compiler_params=pltpu.CompilerParams(
            collective_id=0, has_side_effects=True, vmem_limit_bytes=58 << 20
        ),
    )(
        query_hidden, passage_hidden_rows, weight, bias, query_mask, passage_mask, positives
    )
    return (loss[0, 0], query_grad, passage_grad)


def solution(mesh):
    placed = (
        P("dp", "vocab"),
        P("dp", "vocab"),
        P(None, ("dp", "vocab")),
        P(("dp", "vocab")),
        P("dp", None),
        P("dp", None),
        P("dp"),
    )
    return jax.shard_map(
        shards,
        mesh=mesh,
        in_specs=placed,
        out_specs=(P(), P("dp", "vocab"), P("dp", "vocab")),
        check_vma=False,
    )
```
